32 devices in a mesh: seq: 8 (over z, x), tp: 4 (over y, core).
Axes of the slice: x: 2, y: 2, z: 4, core: 2. Of those that a mesh axis runs over, the one named last changes fastest.
Arguments:
- queries: bfloat16 [1536, 4096], P('seq', 'tp'), may hold values from -80 to 80
- keys: bfloat16 [1536, 512], P('seq', 'tp'), may hold values from -4 to 4
- values: bfloat16 [1536, 512], P('seq', 'tp'), may hold values from -6 to 6
- segment_ids: int32 [1536], P('seq'), may hold values from 0 to 15, never falling along the last dimension, each value on 1 to 1152 neighbouring positions
- out_weight: bfloat16 [4096, 8192], P('tp', 'seq'), may hold values from -0.09375 to 0.09375
Outputs:
- projected: bfloat16 [1536, 8192], P('seq', 'tp')
The draws below stay inside these ranges and needn't reach their ends.
Inputs may be any that keep to these rules, and one draw needn't show every extreme that they name: `segment_ids`: segment numbers never fall along the sequence and every number from 0 to 15 occurs; no document has more than 1152 tokens and one has exactly that many.
All inputs are finite; a program needn't handle non-finite values.
Results may differ from the reference program's by a relative error of at most 0.012.
Values may be sent and summed in bfloat16 or wider, within the bound.
A program may use at most 128 MiB of HBM per device.

```python
import math
import jax
import jax.numpy as jnp
import numpy as np
from jax import lax

HEADS = 32
KV_HEADS = 4
HEAD_DIM = 128
OUT_WIDTH = 8192
SEGMENTS = 16
TOKENS = 1536
N_TP = 4


def draw_key_field(key):
    base_draw = jax.random.normal(jax.random.fold_in(key, 11), (TOKENS, KV_HEADS * HEAD_DIM), jnp.float32)
    return jnp.clip(base_draw, -4.0, 4.0)


def draw_keys(key, part):
    return draw_key_field(key).astype(jnp.bfloat16)


def draw_queries(key, part):
    fresh_draw = 3.0 * jnp.clip(jax.random.normal(jax.random.fold_in(key, 12), (TOKENS, HEADS * HEAD_DIM), jnp.float32), -6.0, 6.0)
    return fresh_draw.astype(jnp.bfloat16)


def levels(stream_key, dims, pieces, low, top_value):
    level, own = 1.0, jax.random.fold_in(stream_key, 6)
    for dim, parts in pieces:
        heights = jnp.exp(jax.random.uniform(jax.random.fold_in(own, dim), (parts,), jnp.float32, low / len(pieces), top_value / len(pieces)))
        level = level * jnp.repeat(heights, dims[dim] // parts).reshape([-1 if axis == dim else 1 for axis in range(len(dims))])
    return level


def length_profile(amount, total, most, skew):
    loads = [(1 << 20) // math.isqrt(grade ** skew) + 1 for grade in range(2, amount + 1)]
    spare, given = total - most - (amount - 1), [1] * (amount - 1)
    while spare > 0:
        free = [i for i in range(amount - 1) if given[i] < most]
        whole, remaining = sum([loads[i] for i in free]), spare
        for i in free:
            extra = min(most - given[i], max(1, remaining * loads[i] // whole), spare)
            given[i] = given[i] + extra
            spare = spare - extra
    return np.array([most] + given)


def uneven(own_key, amount, total, reach, lean):
    if amount == 2:
        one = jax.random.randint(own_key, (), max(1, total - reach), min(reach, total - 1) + 1)
        return jnp.stack([one, total - one])
    sizes = jnp.asarray(length_profile(amount, total, reach, lean), jnp.int32)
    twos = (amount - 1) // 2
    donor, taker = sizes[1:1 + 2 * twos:2], sizes[2:2 + 2 * twos:2]
    slack = jnp.minimum(donor - 1, reach - taker)
    shifted = jax.random.randint(jax.random.fold_in(own_key, 1), (twos,), 0, 1 << 20) % (slack + 1)
    sizes = sizes.at[1:1 + 2 * twos:2].set(donor - shifted).at[2:2 + 2 * twos:2].set(taker + shifted)
    return sizes[jax.random.permutation(jax.random.fold_in(own_key, 2), amount)]


def centred(stream_key, extent, width, most, split=(), kind=jnp.bfloat16):
    result = jax.random.normal(stream_key, extent, jnp.float32) * width
    if len(split) > 0:
        result = levels(stream_key, extent, split, -0.22, 0.18) * result
    return jnp.clip(result, min=-most, max=most).astype(kind)


def setup_inputs(seed: int = 0) -> dict:
    splits = jax.random.split(jax.random.key(seed), 6)
    return {
        "queries": draw_queries(jax.random.fold_in(splits[5], 71), 0),
        "keys": draw_keys(jax.random.fold_in(splits[5], 71), 0),
        "values": centred(splits[2], (TOKENS, KV_HEADS * HEAD_DIM), 1.0, 6.0, ((0, 8), (1, 4))),
        "segment_ids": jnp.searchsorted(jnp.cumsum(uneven(splits[3], SEGMENTS, TOKENS, 3 * TOKENS // 4, 2)), jnp.arange(TOKENS), side="right").astype(jnp.int32),
        "out_weight": centred(splits[4], (HEADS * HEAD_DIM, OUT_WIDTH), (HEADS * HEAD_DIM) ** -0.5, 0.09375, ((0, 4), (1, 8))),
    }


rope_base = 500000.0
masked_score = -1e+30

def rotate_heads(inputs, positions, head_dim):
    row_count = inputs.shape[0]
    head_count = inputs.shape[1] // head_dim
    half_dim = head_dim // 2
    widened = inputs.astype(jnp.float32).reshape(row_count, head_count, head_dim)
    exponent = jnp.arange(half_dim, dtype=jnp.float32) * (2.0 / head_dim)
    inverse = jnp.power(jnp.float32(rope_base), -exponent)
    angles = positions.astype(jnp.float32)[:, None] * inverse[None, :]
    cosine_table = jnp.cos(angles)[:, None, :]
    sine_table = jnp.sin(angles)[:, None, :]
    first_half = widened[:, :, :half_dim]
    second_half = widened[:, :, half_dim:]
    turned = jnp.concatenate([first_half * cosine_table - second_half * sine_table, second_half * cosine_table + first_half * sine_table], axis=2)
    return turned.reshape(row_count, head_count * head_dim).astype(jnp.bfloat16)

def doc_counts_of(segment_ids, segments):
    labels = jnp.arange(segments, dtype=jnp.int32)
    return lax.optimization_barrier(jnp.sum((segment_ids[None, :] == labels[:, None]).astype(jnp.int32), axis=1))

def first_rows(segment, starts):
    labels = jnp.arange(starts.shape[0], dtype=jnp.int32)
    return lax.optimization_barrier(jnp.sum(jnp.where(segment[:, None] == labels[None, :], starts[None, :], 0), axis=1)).astype(jnp.int32)

def reference(queries, keys, values, segment_ids, out_weight):
    counts = doc_counts_of(segment_ids, SEGMENTS)
    doc_ends = jnp.cumsum(counts).astype(jnp.int32)
    starts = doc_ends - counts
    every_row = jnp.arange(TOKENS, dtype=jnp.int32)
    positions = every_row - first_rows(segment_ids, starts)
    query_rot = rotate_heads(queries, positions, HEAD_DIM)
    key_rot = rotate_heads(keys, positions, HEAD_DIM)
    group_size = HEADS // KV_HEADS
    score_scale = 1.0 / math.sqrt(HEAD_DIM)
    key_full = lax.optimization_barrier(key_rot).astype(jnp.float32).reshape(TOKENS, KV_HEADS, HEAD_DIM)
    value_full = values.astype(jnp.float32).reshape(TOKENS, KV_HEADS, HEAD_DIM)
    query_block = 128 if TOKENS % 128 == 0 else TOKENS

    def attend(block_number):
        first_row = block_number * query_block
        query_tile = lax.dynamic_slice_in_dim(query_rot, first_row, query_block, 0)
        query_tile = lax.optimization_barrier(query_tile).astype(jnp.float32).reshape(query_block, KV_HEADS, group_size, HEAD_DIM)
        query_rows = first_row + jnp.arange(query_block, dtype=jnp.int32)
        query_segs = lax.dynamic_slice_in_dim(segment_ids, first_row, query_block, 0)
        scores = jnp.einsum('tkgd,skd->kgts', query_tile, key_full, precision=lax.Precision.HIGHEST) * score_scale
        visible = (every_row[None, :] <= query_rows[:, None]) & (segment_ids[None, :] == query_segs[:, None])
        scores = jnp.where(visible[None, None], scores, masked_score)
        row_max = lax.optimization_barrier(jnp.max(scores, axis=-1, keepdims=True))
        weights_full = jnp.where(visible[None, None], jnp.exp(scores - row_max), 0.0)
        normalizer = lax.optimization_barrier(jnp.sum(weights_full, axis=-1))
        weights_low = lax.optimization_barrier(weights_full.astype(jnp.bfloat16)).astype(jnp.float32)
        numerator = jnp.einsum('kgts,skd->kgtd', weights_low, value_full, precision=lax.Precision.HIGHEST)
        output = numerator / normalizer[..., None]
        return jnp.transpose(output, (2, 0, 1, 3)).reshape(query_block, HEADS * HEAD_DIM).astype(jnp.bfloat16)
    attended = lax.map(attend, jnp.arange(TOKENS // query_block, dtype=jnp.int32)).reshape(TOKENS, HEADS * HEAD_DIM)
    head_width = HEADS * HEAD_DIM // N_TP
    summed = jnp.zeros((TOKENS, OUT_WIDTH), jnp.float32)
    for shard in range(N_TP):
        term = jnp.dot(attended[:, shard * head_width:(shard + 1) * head_width], out_weight[shard * head_width:(shard + 1) * head_width], preferred_element_type=jnp.float32).astype(jnp.bfloat16)
        summed = summed + lax.optimization_barrier(term).astype(jnp.float32)
    return summed.astype(jnp.bfloat16)
```

```python
import math

import jax
import jax.numpy as jnp
from jax import lax
from jax.sharding import PartitionSpec as P

HEADS = 32
KV_HEADS = 4
HEAD_DIM = 128
SEGMENTS = 16


rope_base = 500000.0
masked_score = -1e30


def rotate_heads(inputs, positions, head_dim):
    row_count = inputs.shape[0]
    head_count = inputs.shape[1] // head_dim
    half_dim = head_dim // 2
    widened = inputs.astype(jnp.float32).reshape(row_count, head_count, head_dim)
    exponent = jnp.arange(half_dim, dtype=jnp.float32) * (2.0 / head_dim)
    inverse = jnp.power(jnp.float32(rope_base), -exponent)
    angles = positions.astype(jnp.float32)[:, None] * inverse[None, :]
    cosine_table = jnp.cos(angles)[:, None, :]
    sine_table = jnp.sin(angles)[:, None, :]
    first_half = widened[:, :, :half_dim]
    second_half = widened[:, :, half_dim:]
    turned = jnp.concatenate(
        [
            first_half * cosine_table - second_half * sine_table,
            second_half * cosine_table + first_half * sine_table,
        ],
        axis=2,
    )
    return turned.reshape(row_count, head_count * head_dim).astype(jnp.bfloat16)


def doc_counts_of(segment_ids, segments):
    labels = jnp.arange(segments, dtype=jnp.int32)
    return jnp.sum((segment_ids[None, :] == labels[:, None]).astype(jnp.int32), axis=1)


def first_rows(segment, starts):
    labels = jnp.arange(starts.shape[0], dtype=jnp.int32)
    return jnp.sum(jnp.where(segment[:, None] == labels[None, :], starts[None, :], 0), axis=1)


def segment_of(global_rows, doc_ends):
    return jnp.sum((doc_ends[None, :] <= global_rows[:, None]).astype(jnp.int32), axis=1)


def block_length(piece_rows):
    for candidate in (256, 128):
        return candidate
    candidate = min(piece_rows, 256)
    while piece_rows % candidate != 0:
        candidate = candidate - 1
    return candidate


def local(queries, keys, values, segment_ids, out_weight):
    row_count = queries.shape[0]
    half_rows = row_count // 2
    seq_count = lax.axis_size("seq")
    tp_count = lax.axis_size("tp")
    my_index = lax.axis_index("seq")
    tp_index = lax.axis_index("tp")
    pair_width = keys.shape[1] + values.shape[1]
    id_rows = -(-row_count // pair_width)
    pad_rows = -(-id_rows // 16) * 16
    ids_low = jnp.pad(segment_ids.astype(jnp.bfloat16), (0, pad_rows * pair_width - row_count))
    packed = jnp.concatenate(
        [jnp.concatenate([keys, values], axis=1), ids_low.reshape(pad_rows, pair_width)], axis=0
    )
    gathered = lax.all_gather(packed, "seq", axis=0, tiled=False)
    both = gathered[:, :row_count].reshape(seq_count * row_count, pair_width)
    value_piece = both[:, keys.shape[1] :]
    all_segs = (
        gathered[:, row_count:]
        .reshape(seq_count, pad_rows * pair_width)[:, :row_count]
        .reshape(seq_count * row_count)
        .astype(jnp.int32)
    )
    totals = doc_counts_of(all_segs, SEGMENTS)
    doc_ends = jnp.cumsum(totals)
    starts = doc_ends - totals
    own_rows = my_index * row_count + jnp.arange(row_count, dtype=jnp.int32)
    positions = own_rows - first_rows(segment_ids, starts)
    query_rot = rotate_heads(queries, positions, HEAD_DIM)
    all_rows = jnp.arange(seq_count * row_count, dtype=jnp.int32)
    key_piece = rotate_heads(
        both[:, : keys.shape[1]], all_rows - first_rows(all_segs, starts), HEAD_DIM
    )
    query_segs = segment_ids
    kv_local = keys.shape[1] // HEAD_DIM
    group_size = HEADS // KV_HEADS
    score_scale = 1.0 / math.sqrt(HEAD_DIM)
    query_halves = []
    for which_half in range(2):
        lower = which_half * half_rows
        query_halves.append(
            (
                query_rot[lower : lower + half_rows].reshape(
                    half_rows, kv_local, group_size, HEAD_DIM
                ),
                own_rows[lower : lower + half_rows],
                query_segs[lower : lower + half_rows],
            )
        )

    def empty_state():
        return (
            jnp.full((kv_local, group_size, half_rows), masked_score, jnp.float32),
            jnp.zeros((kv_local, group_size, half_rows), jnp.float32),
            jnp.zeros((kv_local, group_size, half_rows, HEAD_DIM), jnp.float32),
        )

    def attend_tile(carried, key_tile, value_tile, key_rows):
        key_segs = segment_of(key_rows, doc_ends)
        key_heads = key_tile.reshape(-1, kv_local, HEAD_DIM)
        value_heads = value_tile.reshape(-1, kv_local, HEAD_DIM)
        results = []
        for which_half in range(2):
            query_tile, rows_here, segs_here = query_halves[which_half]
            visible = (key_rows[None, :] <= rows_here[:, None]) & (
                key_segs[None, :] == segs_here[:, None]
            )

            def compute(running, query_tile=query_tile, visible=visible):
                row_max, normalizer, numerator = running
                scores = (
                    jnp.einsum(
                        "tkgd,skd->kgts", query_tile, key_heads, preferred_element_type=jnp.float32
                    )
                    * score_scale
                )
                scores = jnp.where(visible[None, None], scores, masked_score)
                new_max = jnp.maximum(row_max, jnp.max(scores, axis=-1))
                rescale = jnp.exp(row_max - new_max)
                weights_full = jnp.where(
                    visible[None, None], jnp.exp(scores - new_max[..., None]), 0.0
                )
                normalizer = normalizer * rescale + jnp.sum(weights_full, axis=-1)
                weights_low = weights_full.astype(jnp.bfloat16)
                numerator = numerator * rescale[..., None] + jnp.einsum(
                    "kgts,skd->kgtd", weights_low, value_heads, preferred_element_type=jnp.float32
                )
                return (new_max, normalizer, numerator)

            def keep(running):
                return running

            results.append(lax.cond(jnp.any(visible), compute, keep, carried[which_half]))
        return tuple(results)

    initial = (empty_state(), empty_state())
    piece_rows = key_piece.shape[0]
    block_rows = block_length(piece_rows)

    def step(block_number, running):
        offset = block_number * block_rows
        key_tile = lax.dynamic_slice_in_dim(key_piece, offset, block_rows, 0)
        value_tile = lax.dynamic_slice_in_dim(value_piece, offset, block_rows, 0)
        key_rows = offset + jnp.arange(block_rows, dtype=jnp.int32)
        return attend_tile(running, key_tile, value_tile, key_rows)

    final = lax.fori_loop(0, piece_rows // block_rows, step, initial)
    halves_out = []
    for which_half in range(2):
        row_max, normalizer, numerator = final[which_half]
        output = numerator / normalizer[..., None]
        halves_out.append(
            jnp.transpose(output, (2, 0, 1, 3))
            .reshape(half_rows, kv_local * group_size * HEAD_DIM)
            .astype(jnp.bfloat16)
        )
    attended = jnp.concatenate(halves_out, axis=0)
    attended_all = lax.all_gather(attended, "seq", axis=0, tiled=True)
    partial_value = jnp.dot(
        attended_all, out_weight, preferred_element_type=jnp.float32
    ).astype(jnp.bfloat16)
    return spread(partial_value, row_count)


def spread(partial_value, row_count):
    seq_count = lax.axis_size("seq")
    tp_count = lax.axis_size("tp")
    per = seq_count // tp_count
    my_index = lax.axis_index("seq")
    summed = lax.psum_scatter(partial_value, "tp", scatter_dimension=0, tiled=True)
    width = summed.shape[1]
    blocks = summed.reshape(per, row_count, width)
    arrived = []
    for slot in range(per):
        pairs = []
        for j in range(seq_count):
            for k in range(tp_count):
                i = k * per + (slot + j) % per
                pairs.append((j * tp_count + k, i * tp_count + j // per))
        outgoing = lax.dynamic_index_in_dim(blocks, (slot + my_index) % per, 0, keepdims=False)
        arrived.append(lax.ppermute(outgoing, ("seq", "tp"), pairs))
    stacked = jnp.stack(arrived, axis=0)
    order = (my_index - jnp.arange(per, dtype=jnp.int32)) % per
    return jnp.concatenate(
        [lax.dynamic_index_in_dim(stacked, order[c], 0, keepdims=False) for c in range(per)],
        axis=1,
    )


def solution(mesh):
    return jax.shard_map(
        local,
        mesh=mesh,
        in_specs=(P("seq", "tp"), P("seq", "tp"), P("seq", "tp"), P("seq"), P("tp", "seq")),
        out_specs=P("seq", "tp"),
        check_vma=False,
    )
```

```python
import functools
import math

import jax
import jax.numpy as jnp
from jax import lax
from jax.experimental import pallas as pl
from jax.experimental.pallas import tpu as pltpu
from jax.sharding import PartitionSpec as P

HEADS = 32
KV_HEADS = 4
HEAD_DIM = 128
SEGMENTS = 16


rope_base = 500000.0
masked_score = -1e30


def rotate_heads(inputs, positions, head_dim):
    row_count = inputs.shape[0]
    head_count = inputs.shape[1] // head_dim
    half_dim = head_dim // 2
    widened = inputs.astype(jnp.float32).reshape(row_count, head_count, head_dim)
    exponent = jnp.arange(half_dim, dtype=jnp.float32) * (2.0 / head_dim)
    inverse = jnp.power(jnp.float32(rope_base), -exponent)
    angles = positions.astype(jnp.float32)[:, None] * inverse[None, :]
    cosine_table = jnp.cos(angles)[:, None, :]
    sine_table = jnp.sin(angles)[:, None, :]
    first_half = widened[:, :, :half_dim]
    second_half = widened[:, :, half_dim:]
    turned = jnp.concatenate(
        [
            first_half * cosine_table - second_half * sine_table,
            second_half * cosine_table + first_half * sine_table,
        ],
        axis=2,
    )
    return turned.reshape(row_count, head_count * head_dim).astype(jnp.bfloat16)


def doc_counts_of(segment_ids, segments):
    labels = jnp.arange(segments, dtype=jnp.int32)
    return jnp.sum((segment_ids[None, :] == labels[:, None]).astype(jnp.int32), axis=1)


def first_rows(segment, starts):
    labels = jnp.arange(starts.shape[0], dtype=jnp.int32)
    return jnp.sum(jnp.where(segment[:, None] == labels[None, :], starts[None, :], 0), axis=1)


def segment_of(global_rows, doc_ends):
    return jnp.sum((doc_ends[None, :] <= global_rows[:, None]).astype(jnp.int32), axis=1)


def block_length(piece_rows):
    for candidate in (256, 128):
        return candidate
    candidate = min(piece_rows, 256)
    while piece_rows % candidate != 0:
        candidate = candidate - 1
    return candidate


def gather_kernel(members, stride, own_ref, all_ref, send_sems, recv_sems):
    me = lax.axis_index("seq")
    slot = lax.div(me, stride)
    place = lax.rem(me, stride)
    peers = [lax.rem(slot + d, members) * stride + place for d in range(1, members)]
    barrier = pltpu.get_barrier_semaphore()
    for peer in peers:
        pl.semaphore_signal(
            barrier, inc=1, device_id={"seq": peer}, device_id_type=pl.DeviceIdType.MESH
        )
    pl.semaphore_wait(barrier, members - 1)
    copies = []
    for d, peer in enumerate(peers):
        copy = pltpu.make_async_remote_copy(
            src_ref=own_ref,
            dst_ref=all_ref.at[slot],
            send_sem=send_sems.at[d],
            recv_sem=recv_sems.at[d],
            device_id={"seq": peer},
            device_id_type=pl.DeviceIdType.MESH,
        )
        copy.start()
        copies.append(copy)
    all_ref[slot] = own_ref[...]
    for copy in copies:
        copy.wait()


def direct_gather(own, members, stride, collective_id):
    moved = own.size * own.dtype.itemsize * (members - 1)
    return pl.pallas_call(
        functools.partial(gather_kernel, members, stride),
        out_shape=jax.ShapeDtypeStruct((members,) + own.shape, own.dtype),
        in_specs=[pl.BlockSpec(memory_space=pltpu.VMEM)],
        out_specs=pl.BlockSpec(memory_space=pltpu.VMEM),
        scratch_shapes=[
            pltpu.SemaphoreType.DMA((members - 1,)),
            pltpu.SemaphoreType.DMA((members - 1,)),
        ],
        compiler_params=pltpu.CompilerParams(
            collective_id=collective_id, has_side_effects=True
        ),
        cost_estimate=pl.CostEstimate(flops=0, bytes_accessed=20 * moved, transcendentals=0),
    )(own)


def local(queries, keys, values, segment_ids, out_weight):
    row_count = queries.shape[0]
    half_rows = row_count // 2
    seq_count = lax.axis_size("seq")
    tp_count = lax.axis_size("tp")
    my_index = lax.axis_index("seq")
    per = seq_count // tp_count
    pair_width = keys.shape[1] + values.shape[1]
    id_rows = -(-row_count // pair_width)
    pad_rows = -(-id_rows // 16) * 16
    ids_low = jnp.pad(segment_ids.astype(jnp.bfloat16), (0, pad_rows * pair_width - row_count))
    packed = jnp.concatenate(
        [jnp.concatenate([keys, values], axis=1), ids_low.reshape(pad_rows, pair_width)], axis=0
    )
    weight_wide = lax.all_gather(
        out_weight,
        "seq",
        axis=1,
        tiled=True,
        axis_index_groups=[
            [t * per + r for r in range(per)] for t in range(tp_count)
        ],
    )
    gathered = direct_gather(packed, seq_count, 1, 0)
    both = gathered[:, :row_count].reshape(seq_count * row_count, pair_width)
    value_piece = both[:, keys.shape[1] :]
    all_segs = (
        gathered[:, row_count:]
        .reshape(seq_count, pad_rows * pair_width)[:, :row_count]
        .reshape(seq_count * row_count)
        .astype(jnp.int32)
    )
    totals = doc_counts_of(all_segs, SEGMENTS)
    doc_ends = jnp.cumsum(totals)
    starts = doc_ends - totals
    own_rows = my_index * row_count + jnp.arange(row_count, dtype=jnp.int32)
    positions = own_rows - first_rows(segment_ids, starts)
    query_rot = rotate_heads(queries, positions, HEAD_DIM)
    all_rows = jnp.arange(seq_count * row_count, dtype=jnp.int32)
    key_piece = rotate_heads(
        both[:, : keys.shape[1]], all_rows - first_rows(all_segs, starts), HEAD_DIM
    )
    query_segs = segment_ids
    kv_local = keys.shape[1] // HEAD_DIM
    group_size = HEADS // KV_HEADS
    score_scale = 1.0 / math.sqrt(HEAD_DIM)
    query_halves = []
    for which_half in range(2):
        lower = which_half * half_rows
        query_halves.append(
            (
                query_rot[lower : lower + half_rows].reshape(
                    half_rows, kv_local, group_size, HEAD_DIM
                ),
                own_rows[lower : lower + half_rows],
                query_segs[lower : lower + half_rows],
            )
        )

    def empty_state():
        return (
            jnp.full((kv_local, group_size, half_rows), masked_score, jnp.float32),
            jnp.zeros((kv_local, group_size, half_rows), jnp.float32),
            jnp.zeros((kv_local, group_size, half_rows, HEAD_DIM), jnp.float32),
        )

    def attend_tile(carried, key_tile, value_tile, key_rows):
        key_segs = segment_of(key_rows, doc_ends)
        key_heads = key_tile.reshape(-1, kv_local, HEAD_DIM)
        value_heads = value_tile.reshape(-1, kv_local, HEAD_DIM)
        results = []
        for which_half in range(2):
            query_tile, rows_here, segs_here = query_halves[which_half]
            visible = (key_rows[None, :] <= rows_here[:, None]) & (
                key_segs[None, :] == segs_here[:, None]
            )

            def compute(running, query_tile=query_tile, visible=visible):
                row_max, normalizer, numerator = running
                scores = (
                    jnp.einsum(
                        "tkgd,skd->kgts", query_tile, key_heads, preferred_element_type=jnp.float32
                    )
                    * score_scale
                )
                scores = jnp.where(visible[None, None], scores, masked_score)
                new_max = jnp.maximum(row_max, jnp.max(scores, axis=-1))
                rescale = jnp.exp(row_max - new_max)
                weights_full = jnp.where(
                    visible[None, None], jnp.exp(scores - new_max[..., None]), 0.0
                )
                normalizer = normalizer * rescale + jnp.sum(weights_full, axis=-1)
                weights_low = weights_full.astype(jnp.bfloat16)
                numerator = numerator * rescale[..., None] + jnp.einsum(
                    "kgts,skd->kgtd", weights_low, value_heads, preferred_element_type=jnp.float32
                )
                return (new_max, normalizer, numerator)

            def keep(running):
                return running

            results.append(lax.cond(jnp.any(visible), compute, keep, carried[which_half]))
        return tuple(results)

    initial = (empty_state(), empty_state())
    piece_rows = key_piece.shape[0]
    block_rows = block_length(piece_rows)

    def step(block_number, running):
        offset = block_number * block_rows
        key_tile = lax.dynamic_slice_in_dim(key_piece, offset, block_rows, 0)
        value_tile = lax.dynamic_slice_in_dim(value_piece, offset, block_rows, 0)
        key_rows = offset + jnp.arange(block_rows, dtype=jnp.int32)
        return attend_tile(running, key_tile, value_tile, key_rows)

    final = lax.fori_loop(0, piece_rows // block_rows, step, initial)
    halves_out = []
    for which_half in range(2):
        row_max, normalizer, numerator = final[which_half]
        output = numerator / normalizer[..., None]
        halves_out.append(
            jnp.transpose(output, (2, 0, 1, 3))
            .reshape(half_rows, kv_local * group_size * HEAD_DIM)
            .astype(jnp.bfloat16)
        )
    attended = jnp.concatenate(halves_out, axis=0)
    attended_all = direct_gather(attended, tp_count, per, 1).reshape(
        tp_count * row_count, attended.shape[1]
    )
    partial_value = jnp.dot(
        attended_all, weight_wide, preferred_element_type=jnp.float32
    ).astype(jnp.bfloat16)
    summed = lax.psum_scatter(partial_value, "tp", scatter_dimension=0, tiled=True)
    pairs = []
    for t in range(tp_count):
        for r in range(per):
            for k in range(tp_count):
                pairs.append(((t * per + r) * tp_count + k, (k * per + r) * tp_count + t))
    return lax.ppermute(summed, ("seq", "tp"), pairs)


def solution(mesh):
    return jax.shard_map(
        local,
        mesh=mesh,
        in_specs=(P("seq", "tp"), P("seq", "tp"), P("seq", "tp"), P("seq"), P("tp", "seq")),
        out_specs=P("seq", "tp"),
        check_vma=False,
    )
```

```python
import functools
import math

import jax
import jax.numpy as jnp
from jax import lax
from jax.experimental import pallas as pl
from jax.experimental.pallas import tpu as pltpu
from jax.sharding import PartitionSpec as P

HEADS = 32
KV_HEADS = 4
HEAD_DIM = 128
SEGMENTS = 16


rope_base = 500000.0
masked_score = -1e30


def rotate_heads(inputs, positions, head_dim):
    row_count = inputs.shape[0]
    head_count = inputs.shape[1] // head_dim
    half_dim = head_dim // 2
    widened = inputs.astype(jnp.float32).reshape(row_count, head_count, head_dim)
    exponent = jnp.arange(half_dim, dtype=jnp.float32) * (2.0 / head_dim)
    inverse = jnp.power(jnp.float32(rope_base), -exponent)
    angles = positions.astype(jnp.float32)[:, None] * inverse[None, :]
    cosine_table = jnp.cos(angles)[:, None, :]
    sine_table = jnp.sin(angles)[:, None, :]
    first_half = widened[:, :, :half_dim]
    second_half = widened[:, :, half_dim:]
    turned = jnp.concatenate(
        [
            first_half * cosine_table - second_half * sine_table,
            second_half * cosine_table + first_half * sine_table,
        ],
        axis=2,
    )
    return turned.reshape(row_count, head_count * head_dim).astype(jnp.bfloat16)


def doc_counts_of(segment_ids, segments):
    labels = jnp.arange(segments, dtype=jnp.int32)
    return jnp.sum((segment_ids[None, :] == labels[:, None]).astype(jnp.int32), axis=1)


def first_rows(segment, starts):
    labels = jnp.arange(starts.shape[0], dtype=jnp.int32)
    return jnp.sum(jnp.where(segment[:, None] == labels[None, :], starts[None, :], 0), axis=1)


def attend_kernel(
    group_size, limits, query_ref, key_ref, value_ref, qseg_ref, kseg_ref, out_ref, top, total, acc
):
    row_count = query_ref.shape[0]
    block_rows = kseg_ref.shape[2]
    head_count = query_ref.shape[1] // HEAD_DIM
    score_scale = 1.0 / math.sqrt(HEAD_DIM)
    top[...] = jnp.full(top.shape, 0.5 * masked_score, jnp.float32)
    total[...] = jnp.zeros(total.shape, jnp.float32)
    acc[...] = jnp.zeros(acc.shape, jnp.float32)

    def tile(number, unused):
        offset = pl.multiple_of(number * block_rows, block_rows)
        key_rows = offset + lax.broadcasted_iota(jnp.int32, (row_count, block_rows), 1)
        rows = limits[2] + lax.broadcasted_iota(jnp.int32, (row_count, block_rows), 0)
        visible = (key_rows <= rows) & (kseg_ref[number] == qseg_ref[...])
        for head in range(head_count):
            lanes = slice(head * HEAD_DIM, (head + 1) * HEAD_DIM)
            kv = head // group_size
            kv_lanes = slice(kv * HEAD_DIM, (kv + 1) * HEAD_DIM)
            scores = lax.dot_general(
                query_ref[:, lanes],
                key_ref[pl.ds(offset, block_rows), kv_lanes],
                (((1,), (1,)), ((), ())),
                preferred_element_type=jnp.float32,
            )
            scores = jnp.where(visible, scores * score_scale, masked_score)
            old = top[head]
            new = jnp.maximum(old, jnp.max(scores, axis=1, keepdims=True))
            rescale = jnp.exp(old - new)
            weights = jnp.exp(scores - new)
            top[head] = new
            total[head] = total[head] * rescale + jnp.sum(weights, axis=1, keepdims=True)
            acc[head] = acc[head] * rescale + jnp.dot(
                weights.astype(jnp.bfloat16),
                value_ref[pl.ds(offset, block_rows), kv_lanes],
                preferred_element_type=jnp.float32,
            )
        return unused

    lax.fori_loop(limits[0], limits[1], tile, 0)
    for head in range(head_count):
        out_ref[:, head * HEAD_DIM : (head + 1) * HEAD_DIM] = (acc[head] / total[head]).astype(
            out_ref.dtype
        )


def attend(query_rot, key_piece, value_piece, query_segs, key_segs, first_row, first_position):
    row_count = query_rot.shape[0]
    token_count = key_piece.shape[0]
    block_rows = 256 if token_count % 256 == 0 else row_count
    head_count = query_rot.shape[1] // HEAD_DIM
    limits = jnp.stack(
        [
            (first_row - first_position) // block_rows,
            (first_row + row_count - 1) // block_rows + 1,
            first_row,
        ]
    ).astype(jnp.int32)
    vmem = pl.BlockSpec(memory_space=pltpu.VMEM)
    return pl.pallas_call(
        functools.partial(attend_kernel, HEADS // KV_HEADS),
        out_shape=jax.ShapeDtypeStruct(query_rot.shape, query_rot.dtype),
        in_specs=[pl.BlockSpec(memory_space=pltpu.SMEM)] + [vmem] * 5,
        out_specs=vmem,
        scratch_shapes=[
            pltpu.VMEM((head_count, row_count, 1), jnp.float32),
            pltpu.VMEM((head_count, row_count, 1), jnp.float32),
            pltpu.VMEM((head_count, row_count, HEAD_DIM), jnp.float32),
        ],
        cost_estimate=pl.CostEstimate(
            flops=4 * row_count * token_count * query_rot.shape[1],
            bytes_accessed=2 * (query_rot.size * 2 + key_piece.size * 2),
            transcendentals=row_count * token_count * head_count,
        ),
    )(
        limits,
        query_rot,
        key_piece,
        value_piece,
        query_segs[:, None],
        key_segs.reshape(token_count // block_rows, 1, block_rows),
    )


def gather_kernel(members, stride, spread_out, own_ref, all_ref, send_sems, recv_sems):
    me = lax.axis_index("seq")
    slot = lax.div(me, stride)
    place = lax.rem(me, stride)
    peers = [lax.rem(slot + d, members) * stride + place for d in range(1, members)]
    barrier = pltpu.get_barrier_semaphore()
    for peer in peers:
        pl.semaphore_signal(
            barrier, inc=1, device_id={"seq": peer}, device_id_type=pl.DeviceIdType.MESH
        )
    pl.semaphore_wait(barrier, members - 1)
    keep = slot if spread_out is None else spread_out(slot)
    copies = []
    for d, peer in enumerate(peers):
        copy = pltpu.make_async_remote_copy(
            src_ref=own_ref,
            dst_ref=all_ref.at[keep],
            send_sem=send_sems.at[d],
            recv_sem=recv_sems.at[d],
            device_id={"seq": peer},
            device_id_type=pl.DeviceIdType.MESH,
        )
        copy.start()
        copies.append(copy)
    all_ref[keep] = own_ref[...]
    for copy in copies:
        copy.wait()


def direct_gather(own, members, stride, collective_id, spread_out=None):
    moved = own.size * own.dtype.itemsize * (members - 1)
    return pl.pallas_call(
        functools.partial(gather_kernel, members, stride, spread_out),
        out_shape=jax.ShapeDtypeStruct((members,) + own.shape, own.dtype),
        in_specs=[pl.BlockSpec(memory_space=pltpu.VMEM)],
        out_specs=pl.BlockSpec(memory_space=pltpu.VMEM),
        scratch_shapes=[
            pltpu.SemaphoreType.DMA((members - 1,)),
            pltpu.SemaphoreType.DMA((members - 1,)),
        ],
        compiler_params=pltpu.CompilerParams(
            collective_id=collective_id, has_side_effects=True
        ),
        cost_estimate=pl.CostEstimate(flops=0, bytes_accessed=20 * moved, transcendentals=0),
    )(own)


def local(queries, keys, values, segment_ids, out_weight):
    row_count = queries.shape[0]
    seq_count = lax.axis_size("seq")
    tp_count = lax.axis_size("tp")
    my_index = lax.axis_index("seq")
    per = seq_count // tp_count
    pair_width = keys.shape[1] + values.shape[1]
    id_rows = -(-row_count // pair_width)
    pad_rows = -(-id_rows // 16) * 16
    ids_low = jnp.pad(segment_ids.astype(jnp.bfloat16), (0, pad_rows * pair_width - row_count))
    packed = jnp.concatenate(
        [jnp.concatenate([keys, values], axis=1), ids_low.reshape(pad_rows, pair_width)], axis=0
    )
    weight_wide = lax.all_gather(
        out_weight,
        "seq",
        axis=1,
        tiled=True,
        axis_index_groups=[
            [t * per + r for r in range(per)] for t in range(tp_count)
        ],
    )
    gathered = direct_gather(packed, seq_count, 1, 0)
    both = gathered[:, :row_count].reshape(seq_count * row_count, pair_width)
    value_piece = both[:, keys.shape[1] :]
    all_segs = (
        gathered[:, row_count:]
        .reshape(seq_count, pad_rows * pair_width)[:, :row_count]
        .reshape(seq_count * row_count)
        .astype(jnp.int32)
    )
    totals = doc_counts_of(all_segs, SEGMENTS)
    doc_ends = jnp.cumsum(totals)
    starts = doc_ends - totals
    own_rows = my_index * row_count + jnp.arange(row_count, dtype=jnp.int32)
    positions = own_rows - first_rows(segment_ids, starts)
    query_rot = rotate_heads(queries, positions, HEAD_DIM)
    all_rows = jnp.arange(seq_count * row_count, dtype=jnp.int32)
    key_piece = rotate_heads(
        both[:, : keys.shape[1]], all_rows - first_rows(all_segs, starts), HEAD_DIM
    )
    attended = attend(
        query_rot, key_piece, value_piece, segment_ids, all_segs, own_rows[0], positions[0]
    )
    half_count = tp_count // 2 if tp_count % 2 == 0 else tp_count

    def keeper(b):
        return (b % half_count) * (tp_count // half_count) + b // half_count

    attended_all = direct_gather(attended, tp_count, per, 1, keeper).reshape(
        tp_count * row_count, attended.shape[1]
    )
    partial_value = jnp.dot(
        attended_all, weight_wide, preferred_element_type=jnp.float32
    ).astype(jnp.bfloat16)
    summed = lax.psum_scatter(partial_value, "tp", scatter_dimension=0, tiled=True)
    pairs = []
    for t in range(tp_count):
        for r in range(per):
            for b in range(tp_count):
                pairs.append(((t * per + r) * tp_count + keeper(b), (b * per + r) * tp_count + t))
    return lax.ppermute(summed, ("seq", "tp"), pairs)


def solution(mesh):
    return jax.shard_map(
        local,
        mesh=mesh,
        in_specs=(P("seq", "tp"), P("seq", "tp"), P("seq", "tp"), P("seq"), P("tp", "seq")),
        out_specs=P("seq", "tp"),
        check_vma=False,
    )
```
